256 devices in a mesh: cluster: 64 (over x, z, core), dir: 4 (over y).
Axes of the slice: x: 4, y: 4, z: 8, core: 2. Of those that a mesh axis runs over, the one named last changes fastest.
Arguments:
- ray_code: int32 [1024, 524288], P('dir', 'cluster'), may hold values from 0 to 16, as said below
- occluder_list: int32 [64, 16], replicated, may hold values from 0 to 511, as said below
- list_count: int32 [64], replicated, may hold values from 1 to 16, 768 in all
- normal_azimuth: float32 [524288], P('cluster'), may hold values from -3.140625 to 3.140625
- normal_height: float32 [524288], P('cluster'), may hold values from -1 to 1
- albedo: float32 [524288], P('cluster'), may hold values from 0.2 to 1
- occluder_exit_radiance: bfloat16 [512, 81, 1024], P('cluster', None, 'dir'), may hold values from -18 to 18
Outputs:
- transfer: bfloat16 [81, 524288], P(None, ('cluster', 'dir'))
The draws below stay inside these ranges and needn't reach their ends.
Inputs may be any that keep to these rules, and one draw needn't show every extreme that they name: `occluder_list`: each row names 16 different blocks, exactly 2 held by each of 8 different clusters; block b is held by cluster b // 8. `list_count`: entry c is the number of leading slots of row c of occluder_list in use. `ray_code`: A code of a vertex of cluster c below list_count[c] names the slot of that cluster's list whose block the ray ends on; any other code means the ray escapes.
All inputs are finite; a program needn't handle non-finite values.
Results may differ from the reference program's by a relative error of at most 0.0041.
Values may be sent and summed in bfloat16 or wider, within the bound.
A program may use at most 128 MiB of HBM per device.

```python
import math
import jax
import jax.numpy as jnp
import numpy as np
from jax import lax

NDIR = 1024
SHORD = 9
LIST_SLOTS = 16
PER_OWNER = 2
BLK_DEV = 8
VERT_DEV = 8192
CLUSTERS = 64
VERTS = 524288
BLOCKS = 512
COEFFS = 81


def owner_draw(owner_key):
    return jax.random.permutation(owner_key, CLUSTERS)[:LIST_SLOTS // PER_OWNER]


def inner_draw(inner_key):
    return jax.random.permutation(inner_key, BLK_DEV)[:PER_OWNER]


def order_draw(order_key):
    return jax.random.permutation(order_key, LIST_SLOTS)


def draw_occluder_list(key, part):
    groups = LIST_SLOTS // PER_OWNER
    owner_keys = jax.random.split(jax.random.fold_in(key, 11), CLUSTERS)
    owners = jax.vmap(owner_draw)(owner_keys)
    inner_keys = jax.random.split(jax.random.fold_in(key, 12), CLUSTERS * groups)
    inner = jax.vmap(inner_draw)(inner_keys).reshape(CLUSTERS, groups, PER_OWNER)
    entries = (owners[:, :, None] * BLK_DEV + inner).reshape(CLUSTERS, LIST_SLOTS)
    order_keys = jax.random.split(jax.random.fold_in(key, 13), CLUSTERS)
    orders = jax.vmap(order_draw)(order_keys)
    return jnp.take_along_axis(entries, orders, axis=1).astype(jnp.int32)


def draw_ray_code(key, part):
    raw = jax.random.randint(jax.random.fold_in(key, 21), (NDIR, VERTS), 0, 2 * LIST_SLOTS)
    return jnp.minimum(raw, LIST_SLOTS).astype(jnp.int32)


def levels(key, dims, shards, smallest, top_value):
    def one(axis_at, blocks):
        heights = jax.random.uniform(jax.random.fold_in(jax.random.fold_in(key, 6), axis_at), (blocks,), jnp.float32, smallest / len(shards), top_value / len(shards))
        return jnp.repeat(jnp.exp(heights), dims[axis_at] // blocks).reshape((-1,) + (1,) * (len(dims) - axis_at - 1))

    gain = one(*shards[0])
    for cut in shards[1:]:
        gain = gain * one(*cut)
    return gain


def profile(count, total, reach, lean):
    portions = [(1 << 20) // math.isqrt(standing ** lean) + 1 for standing in range(2, count + 1)]
    rest, counts = total - reach - (count - 1), [1] * (count - 1)
    while rest > 0:
        free = [i for i in range(count - 1) if counts[i] < reach]
        pool, budget = sum([portions[i] for i in free]), rest
        for i in free:
            more = min(reach - counts[i], max(1, budget * portions[i] // pool), rest)
            counts[i] = counts[i] + more
            rest = rest - more
    return np.array([reach] + counts)


def ragged_sizes(stream_key, count, total, bound, slope):
    if count == 2:
        one = jax.random.randint(stream_key, (), max(1, total - bound), min(bound, total - 1) + 1)
        return jnp.stack([one, total - one])
    lengths = jnp.asarray(profile(count, total, bound, slope), jnp.int32)
    twos = (count - 1) // 2
    giver, taker = lengths[1:1 + 2 * twos:2], lengths[2:2 + 2 * twos:2]
    room = jnp.minimum(giver - 1, bound - taker)
    shifted = jax.random.randint(jax.random.fold_in(stream_key, 1), (twos,), 0, 1 << 20) % (room + 1)
    lengths = lengths.at[1:1 + 2 * twos:2].set(giver - shifted).at[2:2 + 2 * twos:2].set(taker + shifted)
    return lengths[jax.random.permutation(jax.random.fold_in(stream_key, 2), count)]


def noise(stream_key, shape, deviation, limit, cuts=(), kind=jnp.bfloat16):
    result = deviation * jax.random.normal(stream_key, shape, jnp.float32)
    if cuts:
        result = result * levels(stream_key, shape, cuts, -0.22, 0.18)
    return jnp.clip(result, -limit, limit).astype(kind)


def setup_inputs(seed: int = 0) -> dict:
    arg_keys = jax.random.split(jax.random.key(seed), 8)
    ray_code = draw_ray_code(jax.random.fold_in(arg_keys[7], 71), 0)
    occluder_list = draw_occluder_list(jax.random.fold_in(arg_keys[7], 71), 0)
    list_count = ragged_sizes(arg_keys[2], CLUSTERS, CLUSTERS * 3 * LIST_SLOTS // 4, LIST_SLOTS, 2).astype(jnp.int32)
    normal_azimuth = jnp.clip(jax.random.uniform(arg_keys[3], (VERTS,), jnp.float32, -3.140625, 3.140625), -3.140625, 3.140625)
    normal_height = jnp.clip(jax.random.uniform(arg_keys[4], (VERTS,), jnp.float32, -1.0, 1.0) * levels(arg_keys[4], (VERTS,), ((0, 64),), -0.4, 0.0), -1.0, 1.0)
    albedo = jnp.clip(jnp.exp(math.log(1.0) - 1.609438 * jax.random.uniform(arg_keys[5], (VERTS,), jnp.float32) ** levels(arg_keys[5], (VERTS,), ((0, 64),), -0.2, 0.2)), 0.2, 1.0)
    occluder_exit_radiance = noise(arg_keys[6], (BLOCKS, COEFFS, NDIR), 3.0, 18.0, ((0, 64), (2, 4)))
    return dict(ray_code=ray_code, occluder_list=occluder_list, list_count=list_count, normal_azimuth=normal_azimuth, normal_height=normal_height, albedo=albedo, occluder_exit_radiance=occluder_exit_radiance)


golden_angle = math.pi * (3.0 - math.sqrt(5.0))

def sphere_points(direction_index, direction_overall_count):
    position = direction_index.astype(jnp.float32)
    along_z = 1.0 - (2.0 * position + 1.0) / direction_overall_count
    radius = jnp.sqrt(jnp.maximum(1.0 - along_z * along_z, 0.0))
    turned = position * golden_angle
    return (radius * jnp.cos(turned), radius * jnp.sin(turned), along_z)

def harmonic_table(along_x, along_y, along_z, degrees):
    cosine_terms = [jnp.ones_like(along_x)]
    sine_terms = [jnp.zeros_like(along_x)]
    for power_exponent in range(1, degrees):
        cosine_terms.append(cosine_terms[-1] * along_x - sine_terms[-1] * along_y)
        sine_terms.append(cosine_terms[-2] * along_y + sine_terms[-1] * along_x)
    basis_rows = [None] * (degrees * degrees)
    for order_index in range(degrees):
        diagonal_entries = 1.0
        for factor in range(1, 2 * order_index, 2):
            diagonal_entries = diagonal_entries * factor
        legendre = [None] * degrees
        legendre[order_index] = jnp.full_like(along_z, diagonal_entries)
        if order_index + 1 < degrees:
            legendre[order_index + 1] = along_z * ((2 * order_index + 1) * diagonal_entries)
        for degree in range(order_index + 2, degrees):
            legendre[degree] = ((2 * degree - 1) * along_z * legendre[degree - 1] - (degree + order_index - 1) * legendre[degree - 2]) / (degree - order_index)
        for degree in range(order_index, degrees):
            factor_norm = math.sqrt((2 * degree + 1) / (4.0 * math.pi) * math.factorial(degree - order_index) / math.factorial(degree + order_index))
            centre = degree * degree + degree
            if order_index == 0:
                basis_rows[centre] = factor_norm * legendre[degree]
            else:
                basis_rows[centre + order_index] = math.sqrt(2.0) * factor_norm * legendre[degree] * cosine_terms[order_index]
                basis_rows[centre - order_index] = math.sqrt(2.0) * factor_norm * legendre[degree] * sine_terms[order_index]
    return jnp.stack(basis_rows)

def facing_table(normal_azimuth, normal_height, along_x, along_y, along_z):
    planar = jnp.sqrt(jnp.maximum(1.0 - normal_height * normal_height, 0.0))
    normal_x = planar * jnp.cos(normal_azimuth)
    normal_y = planar * jnp.sin(normal_azimuth)
    return jnp.maximum(along_x[:, None] * normal_x[None, :] + along_y[:, None] * normal_y[None, :] + along_z[:, None] * normal_height[None, :], 0.0)

def reference(ray_code, occluder_list, list_count, normal_azimuth, normal_height, albedo, occluder_exit_radiance):
    along_x, along_y, along_z = sphere_points(lax.iota(jnp.int32, NDIR), NDIR)
    harmonics = harmonic_table(along_x, along_y, along_z, SHORD)
    dir_block = min(64, NDIR)

    def per_cluster(group_cluster_index):
        first_vertex = (group_cluster_index * VERT_DEV).astype(jnp.int32)
        ray_codes = lax.dynamic_slice_in_dim(ray_code, first_vertex, VERT_DEV, 1)
        azimuths = lax.dynamic_slice_in_dim(normal_azimuth, first_vertex, VERT_DEV, 0)
        height_values = lax.dynamic_slice_in_dim(normal_height, first_vertex, VERT_DEV, 0)
        albedos = lax.dynamic_slice_in_dim(albedo, first_vertex, VERT_DEV, 0)
        facing = facing_table(azimuths, height_values, along_x, along_y, along_z)
        live_count = list_count[group_cluster_index]
        occluded = ray_codes < live_count
        direct = jnp.dot(harmonics, jnp.where(occluded, 0.0, facing), precision=lax.Precision.HIGHEST, preferred_element_type=jnp.float32)
        rounded = jnp.where(occluded, facing, 0.0).astype(jnp.bfloat16)
        weight = lax.optimization_barrier(rounded).astype(jnp.float32)
        entries = jnp.take(occluder_exit_radiance, occluder_list[group_cluster_index], axis=0).astype(jnp.float32)
        by_dir = jnp.transpose(entries, (2, 0, 1))
        safe_codes = jnp.minimum(ray_codes, LIST_SLOTS - 1)

        def add_block(block_index, total):
            first_dir = (block_index * dir_block).astype(jnp.int32)
            table = lax.dynamic_slice_in_dim(by_dir, first_dir, dir_block, 0)
            picks = lax.dynamic_slice_in_dim(safe_codes, first_dir, dir_block, 0)
            lit = lax.dynamic_slice_in_dim(weight, first_dir, dir_block, 0)
            gathered = jnp.take_along_axis(table, picks[:, :, None], axis=1)
            return total + jnp.einsum('dv,dvk->kv', lit, gathered, precision=lax.Precision.HIGHEST)
        bounce = lax.fori_loop(0, NDIR // dir_block, add_block, jnp.zeros((COEFFS, VERT_DEV), jnp.float32))
        return 4.0 * math.pi / NDIR * (direct + albedos[None, :] * bounce)
    results = lax.map(per_cluster, lax.iota(jnp.int32, CLUSTERS))
    return jnp.transpose(results, (1, 0, 2)).reshape(COEFFS, VERTS).astype(jnp.bfloat16)
```

```python
import functools
import math

import jax
import jax.numpy as jnp
import numpy as np
from jax import lax
from jax.experimental import pallas as pl
from jax.experimental.pallas import tpu as pltpu
from jax.sharding import PartitionSpec as P

NDIR = 1024
SHORD = 9
COEFFS = 81
SLOTS = 16
CLUSTERS = 64
BLK = 8
DIRS = 256
HALF = 128
VERTS = 8192
OWN = 2048
KG = 32
PARTS = 3
ROWS = KG * PARTS
SEND = 88
NB = 1024
NI = 256
F32 = jnp.float32
BF16 = jnp.bfloat16
MESH = pl.DeviceIdType.MESH
GOLDEN = math.pi * (3.0 - math.sqrt(5.0))


def direction_tables():
    p = np.arange(NDIR, dtype=np.float32)
    z = (np.float32(1.0) - (np.float32(2.0) * p + np.float32(1.0)) / np.float32(NDIR)).astype(np.float32)
    r = np.sqrt(np.maximum(np.float32(1.0) - z * z, np.float32(0.0)))
    t = (p * np.float32(GOLDEN)).astype(np.float64)
    x = (r * np.cos(t).astype(np.float32)).astype(np.float64)
    y = (r * np.sin(t).astype(np.float32)).astype(np.float64)
    z = z.astype(np.float64)
    c, s = [np.ones_like(x)], [np.zeros_like(x)]
    for _ in range(1, SHORD):
        c.append(c[-1] * x - s[-1] * y)
        s.append(c[-2] * y + s[-1] * x)
    rows = [None] * COEFFS
    for m in range(SHORD):
        q = [None] * SHORD
        q[m] = np.full_like(z, float(np.prod(np.arange(1, 2 * m, 2, dtype=np.float64))))
        if m + 1 < SHORD:
            q[m + 1] = z * (2 * m + 1) * q[m]
        for l in range(m + 2, SHORD):
            q[l] = ((2 * l - 1) * z * q[l - 1] - (l + m - 1) * q[l - 2]) / (l - m)
        for l in range(m, SHORD):
            n = math.sqrt((2 * l + 1) / (4.0 * math.pi) * math.factorial(l - m) / math.factorial(l + m))
            at = l * l + l
            if m == 0:
                rows[at] = n * q[l]
            else:
                rows[at + m] = math.sqrt(2.0) * n * q[l] * c[m]
                rows[at - m] = math.sqrt(2.0) * n * q[l] * s[m]
    table = np.zeros((4, ROWS, DIRS), np.float32)
    table[:, :COEFFS] = np.stack(rows).reshape(COEFFS, 4, DIRS).transpose(1, 0, 2)
    axes = np.zeros((4, DIRS, 8), np.float32)
    for i, a in enumerate((x, y, z)):
        axes[:, :, i] = a.reshape(4, DIRS)
    return table, axes


def place(cluster):
    chip = cluster // 2
    spread = (chip % 8) * 4 + chip // 8
    return cluster % 2, (spread * 5) % KG


def fetch_kernel(block_ref, list_ref, out_ref, slices, picked, table, send1, recv1, send2, recv2):
    me = lax.axis_index("cluster")
    my_half, my_group = place(me)
    barrier = pltpu.get_barrier_semaphore()

    def greet(i, carry):
        pl.semaphore_signal(
            barrier, inc=1, device_id={"cluster": (me + i) % CLUSTERS}, device_id_type=MESH
        )
        return carry

    lax.fori_loop(1, CLUSTERS, greet, 0)
    slices[me] = block_ref[my_half, my_group]
    pl.semaphore_wait(barrier, CLUSTERS - 1)

    def first(i):
        peer = (me + i) % CLUSTERS
        half, group = place(peer)
        return pltpu.make_async_remote_copy(
            src_ref=block_ref.at[half, group],
            dst_ref=slices.at[me],
            send_sem=send1,
            recv_sem=recv1,
            device_id={"cluster": peer},
            device_id_type=MESH,
        )

    def start_first(i, carry):
        first(i).start()
        return carry

    lax.fori_loop(1, CLUSTERS, start_first, 0)
    chosen = jnp.where(
        list_ref[...] == lax.broadcasted_iota(jnp.int32, (CLUSTERS * SLOTS, CLUSTERS * BLK), 1), 1.0, 0.0
    ).astype(BF16)
    others = slices.at[pl.ds(0, CLUSTERS - 1)]
    pltpu.make_async_copy(others, others, recv1).wait()
    for part in range(PARTS):
        held = slices[:, part].reshape(CLUSTERS * BLK, HALF)
        rows = jnp.dot(chosen, held, preferred_element_type=F32).astype(BF16)
        picked[:, part] = rows.reshape(CLUSTERS, SLOTS, HALF)
    table[my_half, my_group] = picked[me]

    def second(i):
        peer = (me + i) % CLUSTERS
        return pltpu.make_async_remote_copy(
            src_ref=picked.at[peer],
            dst_ref=table.at[my_half, my_group],
            send_sem=send2,
            recv_sem=recv2,
            device_id={"cluster": peer},
            device_id_type=MESH,
        )

    def start_second(i, carry):
        second(i).start()
        return carry

    lax.fori_loop(1, CLUSTERS, start_second, 0)
    to = lax.broadcasted_iota(jnp.int32, (SLOTS * KG, SLOTS * KG), 0)
    fro = lax.broadcasted_iota(jnp.int32, (SLOTS * KG, SLOTS * KG), 1)
    turn = jnp.where((to % KG) * SLOTS + to // KG == fro, 1.0, 0.0).astype(BF16)
    pltpu.make_async_copy(others, others, send1).wait()
    sent = picked.at[pl.ds(0, CLUSTERS - 1)]
    pltpu.make_async_copy(sent, sent, send2).wait()
    pltpu.make_async_copy(sent, sent, recv2).wait()
    for part in range(PARTS):
        for half in range(2):
            got = table[half, :, part].reshape(KG * SLOTS, HALF)
            turned = jnp.dot(turn, got, preferred_element_type=F32).astype(BF16)
            out_ref[:, part * KG : (part + 1) * KG, half * HALF : (half + 1) * HALF] = turned.reshape(
                SLOTS, KG, HALF
            )


def compute_kernel(
    code_ref, count_ref, axes_ref, vert_ref, harm_ref, table_ref, out_ref,
    codes, total, parts, got, code_sem, send_sem, recv_sem,
):
    me = lax.axis_index("dir")
    cluster = lax.axis_index("cluster")
    steps = VERTS // NB
    per = OWN // NB

    def first_of(t):
        return pl.multiple_of(((me + 1 + t // per) % 4) * OWN + (t % per) * NB, NB)

    def fetch(t):
        return pltpu.make_async_copy(code_ref.at[:, pl.ds(first_of(t), NB)], codes.at[t], code_sem.at[t])

    for t in range(steps):
        fetch(t).start()
    barrier = pltpu.get_barrier_semaphore()
    for i in range(1, 4):
        pl.semaphore_signal(barrier, inc=1, device_id={"dir": (me + i) % 4}, device_id_type=MESH)
    pl.semaphore_wait(barrier, 3)
    count = count_ref[cluster]
    x, y, z = (axes_ref[me, :, i : i + 1] for i in range(3))

    def exchange(t):
        owner = t // per
        return pltpu.make_async_remote_copy(
            src_ref=parts.at[t],
            dst_ref=got.at[t],
            send_sem=send_sem.at[t],
            recv_sem=recv_sem.at[t],
            device_id={"dir": (me + 1 + owner) % 4},
            device_id_type=MESH,
        )

    def step(t, carry):
        fetch(t).wait()
        base = first_of(t)
        for n in range(NB // NI):
            cols = slice(n * NI, (n + 1) * NI)
            vert = vert_ref[:, pl.ds(pl.multiple_of(base + n * NI, NI), NI)]
            code = codes[t, :, cols]
            facing = jnp.maximum(x * vert[0:1] + y * vert[1:2] + z * vert[2:3], 0.0)
            hit = code < count
            lit = jnp.where(hit, 0.0, facing).astype(BF16)
            weight = facing.astype(BF16)
            slot = jnp.where(hit, code, SLOTS).astype(jnp.int16)
            bounce = None
            for s in range(SLOTS):
                spread = jnp.where(slot == jnp.int16(s), weight, jnp.zeros_like(weight))
                term = jnp.dot(table_ref[s], spread, preferred_element_type=F32)
                bounce = term if bounce is None else bounce + term
            direct = jnp.dot(harm_ref[me], lit, preferred_element_type=F32)
            total[t % per, :, cols] = (4.0 * math.pi / NDIR) * (direct + vert[3:4] * bounce)

        @pl.when(t < steps - per)
        def _():
            parts[t] = total[t % per, :SEND].astype(BF16)
            exchange(t).start()

        return carry

    lax.fori_loop(0, steps, step, 0)
    for t in range(steps - per):
        exchange(t).wait()
    for h in range(per):
        mine = total[h, :SEND]
        for i in range(3):
            mine = mine + got[i * per + h].astype(F32)
        out_ref[:, h * NB : (h + 1) * NB] = mine[:COEFFS].astype(BF16)


def per_device(
    ray_code, occluder_list, list_count, normal_azimuth, normal_height, albedo, occluder_exit_radiance
):
    table, axes = direction_tables()
    blocks = jnp.pad(occluder_exit_radiance, ((0, 0), (0, ROWS - COEFFS), (0, 0)))
    blocks = blocks.reshape(BLK, PARTS, KG, 2, HALF).transpose(3, 2, 1, 0, 4)
    planar = jnp.sqrt(jnp.maximum(1.0 - normal_height * normal_height, 0.0))
    verts = jnp.stack(
        [planar * jnp.cos(normal_azimuth), planar * jnp.sin(normal_azimuth), normal_height, albedo]
    )
    vmem = pl.BlockSpec(memory_space=pltpu.VMEM)
    tables = pl.pallas_call(
        fetch_kernel,
        out_shape=jax.ShapeDtypeStruct((SLOTS, ROWS, DIRS), BF16),
        in_specs=[vmem, vmem],
        out_specs=vmem,
        scratch_shapes=[
            pltpu.VMEM((CLUSTERS, PARTS, BLK, HALF), BF16),
            pltpu.VMEM((CLUSTERS, PARTS, SLOTS, HALF), BF16),
            pltpu.VMEM((2, KG, PARTS, SLOTS, HALF), BF16),
            pltpu.SemaphoreType.DMA,
            pltpu.SemaphoreType.DMA,
            pltpu.SemaphoreType.DMA,
            pltpu.SemaphoreType.DMA,
        ],
        compiler_params=pltpu.CompilerParams(
            collective_id=0, has_side_effects=True, vmem_limit_bytes=32 << 20
        ),
        name="fetch",
    )(blocks, occluder_list.reshape(CLUSTERS * SLOTS, 1))
    steps, per = VERTS // NB, OWN // NB
    return pl.pallas_call(
        compute_kernel,
        out_shape=jax.ShapeDtypeStruct((COEFFS, OWN), BF16),
        in_specs=[
            pl.BlockSpec(memory_space=pl.ANY),
            pl.BlockSpec(memory_space=pltpu.SMEM),
            vmem, vmem, vmem, vmem,
        ],
        out_specs=vmem,
        scratch_shapes=[
            pltpu.VMEM((steps, DIRS, NB), jnp.int32),
            pltpu.VMEM((per, ROWS, NB), F32),
            pltpu.VMEM((steps - per, SEND, NB), BF16),
            pltpu.VMEM((steps - per, SEND, NB), BF16),
            pltpu.SemaphoreType.DMA((steps,)),
            pltpu.SemaphoreType.DMA((steps - per,)),
            pltpu.SemaphoreType.DMA((steps - per,)),
        ],
        compiler_params=pltpu.CompilerParams(
            collective_id=1, has_side_effects=True, vmem_limit_bytes=56 << 20
        ),
        name="transfer",
    )(ray_code, list_count, jnp.asarray(axes), verts, jnp.asarray(table).astype(BF16), tables)


def solution(mesh):
    return jax.shard_map(
        per_device,
        mesh=mesh,
        in_specs=(
            P("dir", "cluster"),
            P(),
            P(),
            P("cluster"),
            P("cluster"),
            P("cluster"),
            P("cluster", None, "dir"),
        ),
        out_specs=P(None, ("cluster", "dir")),
        check_vma=False,
    )
```

```python
import math

import jax
import jax.numpy as jnp
import numpy as np
from jax import lax
from jax.experimental import pallas as pl
from jax.experimental.pallas import tpu as pltpu
from jax.sharding import PartitionSpec as P

NDIR = 1024
SHORD = 9
COEFFS = 81
SLOTS = 16
CLUSTERS = 64
BLK = 8
DIRS = 256
HALF = 128
VERTS = 8192
OWN = 2048
KG = 32
PARTS = 3
ROWS = KG * PARTS
SEND = 88
FULL = COEFFS - KG * (PARTS - 1)
NB = 1024
NI = 256
F32 = jnp.float32
BF16 = jnp.bfloat16
MESH = pl.DeviceIdType.MESH
SCALE = 4.0 * math.pi / NDIR
GOLDEN = math.pi * (3.0 - math.sqrt(5.0))


def direction_tables():
    p = np.arange(NDIR, dtype=np.float32)
    z = (np.float32(1.0) - (np.float32(2.0) * p + np.float32(1.0)) / np.float32(NDIR)).astype(np.float32)
    r = np.sqrt(np.maximum(np.float32(1.0) - z * z, np.float32(0.0)))
    t = (p * np.float32(GOLDEN)).astype(np.float64)
    x = (r * np.cos(t).astype(np.float32)).astype(np.float64)
    y = (r * np.sin(t).astype(np.float32)).astype(np.float64)
    z = z.astype(np.float64)
    c, s = [np.ones_like(x)], [np.zeros_like(x)]
    for _ in range(1, SHORD):
        c.append(c[-1] * x - s[-1] * y)
        s.append(c[-2] * y + s[-1] * x)
    rows = [None] * COEFFS
    for m in range(SHORD):
        q = [None] * SHORD
        q[m] = np.full_like(z, float(np.prod(np.arange(1, 2 * m, 2, dtype=np.float64))))
        if m + 1 < SHORD:
            q[m + 1] = z * (2 * m + 1) * q[m]
        for l in range(m + 2, SHORD):
            q[l] = ((2 * l - 1) * z * q[l - 1] - (l + m - 1) * q[l - 2]) / (l - m)
        for l in range(m, SHORD):
            n = math.sqrt((2 * l + 1) / (4.0 * math.pi) * math.factorial(l - m) / math.factorial(l + m))
            at = l * l + l
            if m == 0:
                rows[at] = n * q[l]
            else:
                rows[at + m] = math.sqrt(2.0) * n * q[l] * c[m]
                rows[at - m] = math.sqrt(2.0) * n * q[l] * s[m]
    table = np.zeros((4, ROWS, DIRS), np.float32)
    table[:, :COEFFS] = np.stack(rows).reshape(COEFFS, 4, DIRS).transpose(1, 0, 2)
    axes = np.zeros((4, DIRS, 8), np.float32)
    for i, a in enumerate((x, y, z)):
        axes[:, :, i] = a.reshape(4, DIRS)
    return table, axes


def place(cluster):
    chip = lax.div(cluster, 2)
    spread = lax.rem(chip, 8) * 4 + lax.div(chip, 8)
    return lax.rem(cluster, 2), lax.rem(spread * 5, KG)


def transfer_kernel(
    code_ref, count_ref, block_ref, list_ref, axes_ref, azimuth_ref, height_ref, albedo_ref, harm_ref, out_ref,
    codes, weight, slot, direct, total, normal, chosen, turn, slices, picked, table, matrix, parts, got,
    code_sem, send_a, send_b, recv_a, recv_b, send_c, send_d, recv_c, recv_d, send_sem, recv_sem,
):
    me = lax.axis_index("cluster")
    row = lax.axis_index("dir")
    my_half, my_group = place(me)
    steps = VERTS // NB

    def first_of(t):
        pair, half = lax.div(t, 2), lax.rem(t, 2)
        ahead = lax.rem(2 + pair, 4) + lax.div(pair, 2) * (1 - 2 * lax.rem(pair, 2))
        ahead = ahead + 2 * half * lax.rem(lax.div(pair + 1, 2), 2)
        return pl.multiple_of(lax.rem(row + ahead, 4) * OWN + half * NB, NB)

    def fetch(t):
        return pltpu.make_async_copy(code_ref.at[:, pl.ds(first_of(t), NB)], codes.at[t], code_sem.at[t])

    def start_fetch(t, carry):
        fetch(t).start()
        return carry

    lax.fori_loop(0, steps, start_fetch, 0)
    barrier = pltpu.get_barrier_semaphore()

    def greet(i, carry):
        pl.semaphore_signal(
            barrier, inc=1, device_id={"cluster": lax.rem(me + i, CLUSTERS)}, device_id_type=MESH
        )
        return carry

    lax.fori_loop(1, CLUSTERS, greet, 0)
    for i in (1, 3):
        pl.semaphore_signal(barrier, inc=1, device_id={"dir": lax.rem(row + i, 4)}, device_id_type=MESH)

    slices[me] = block_ref[my_half, my_group]
    chosen[...] = jnp.where(
        list_ref[...] == lax.broadcasted_iota(jnp.int32, (CLUSTERS * SLOTS, CLUSTERS * BLK), 1), 1.0, 0.0
    ).astype(BF16)
    to = lax.broadcasted_iota(jnp.int32, (SLOTS * KG, SLOTS * KG), 0)
    fro = lax.broadcasted_iota(jnp.int32, (SLOTS * KG, SLOTS * KG), 1)
    turn[...] = jnp.where((to % KG) * SLOTS + to // KG == fro, 1.0, 0.0).astype(BF16)
    table[:, FULL:, PARTS - 1] = jnp.zeros((2, KG - FULL, SLOTS, HALF), BF16)
    height = height_ref[...]
    planar = jnp.sqrt(jnp.maximum(1.0 - height * height, 0.0))
    normal[0] = planar * jnp.cos(azimuth_ref[...])
    normal[1] = planar * jnp.sin(azimuth_ref[...])
    pl.semaphore_wait(barrier, CLUSTERS + 1)

    def first(i, lead):
        peer = lax.rem(me + i, CLUSTERS)
        half, group = place(peer)
        units = pl.ds(0, PARTS - 1) if lead else pl.ds(PARTS - 1, 1)
        return group, pltpu.make_async_remote_copy(
            src_ref=block_ref.at[half, group, units],
            dst_ref=slices.at[me, units],
            send_sem=send_a if lead else send_b,
            recv_sem=recv_a if lead else recv_b,
            device_id={"cluster": peer},
            device_id_type=MESH,
        )

    def start_first(i, carry):
        first(i, True)[1].start()
        return carry

    def start_first_rest(i, carry):
        group, copy = first(i, False)

        @pl.when(group < FULL)
        def _():
            copy.start()

        return carry

    lax.fori_loop(1, CLUSTERS, start_first, 0)
    lax.fori_loop(1, CLUSTERS, start_first_rest, 0)

    count = count_ref[me]
    x, y, z = (axes_ref[row, :, i : i + 1] for i in range(3))

    def across(ref, at):
        return jnp.concatenate([ref[pl.ds(at + i, 1), :] for i in range(NI // HALF)], axis=1)

    def prepare(t, carry):
        fetch(t).wait()
        base = lax.div(first_of(t), HALF)
        for n in range(NB // NI):
            cols = slice(n * NI, (n + 1) * NI)
            at = base + n * (NI // HALF)
            code = codes[t, :, cols]
            facing = jnp.maximum(
                x * across(normal.at[0], at) + y * across(normal.at[1], at) + z * across(height_ref, at), 0.0
            )
            hit = code < count
            weight[t, :, cols] = facing.astype(BF16)
            slot[t, :, cols] = jnp.where(hit, code, SLOTS).astype(jnp.int16)
            lit = jnp.where(hit, 0.0, facing)
            high = lit.astype(BF16)
            low = (lit - high.astype(F32)).astype(BF16)
            both = jnp.dot(harm_ref[row], high, preferred_element_type=F32)
            rest = jnp.dot(harm_ref[row, :ROWS], low, preferred_element_type=F32)
            direct[t, :, cols] = SCALE * (both[:ROWS] + both[ROWS:] + rest)
        return carry

    lax.fori_loop(0, 4, prepare, 0)

    others = slices.at[pl.ds(0, CLUSTERS - 1), pl.ds(0, PARTS - 1)]
    pltpu.make_async_copy(others, others, recv_a).wait()
    held = jnp.concatenate([slices[:, i].reshape(CLUSTERS * BLK, HALF) for i in range(PARTS - 1)], axis=1)
    rows = jnp.dot(chosen[...], held, preferred_element_type=F32).astype(BF16)
    for i in range(PARTS - 1):
        picked[:, i] = rows[:, i * HALF : (i + 1) * HALF].reshape(CLUSTERS, SLOTS, HALF)

    def second(i, lead):
        peer = lax.rem(me + i, CLUSTERS)
        units = pl.ds(0, PARTS - 1) if lead else pl.ds(PARTS - 1, 1)
        return pltpu.make_async_remote_copy(
            src_ref=picked.at[peer, units],
            dst_ref=table.at[my_half, my_group, units],
            send_sem=send_c if lead else send_d,
            recv_sem=recv_c if lead else recv_d,
            device_id={"cluster": peer},
            device_id_type=MESH,
        )

    def start_second(i, carry):
        second(i, True).start()
        return carry

    def start_second_rest(i, carry):
        second(i, False).start()
        return carry

    lax.fori_loop(1, CLUSTERS, start_second, 0)
    table[my_half, my_group, : PARTS - 1] = picked[me, : PARTS - 1]
    last = slices.at[pl.ds(0, CLUSTERS - 1), pl.ds(PARTS - 1, 1)]

    @pl.when(my_group < FULL)
    def _():
        pltpu.make_async_copy(last, last, recv_b).wait()
        held = slices[:, PARTS - 1].reshape(CLUSTERS * BLK, HALF)
        rows = jnp.dot(chosen[...], held, preferred_element_type=F32).astype(BF16)
        picked[:, PARTS - 1] = rows.reshape(CLUSTERS, SLOTS, HALF)
        lax.fori_loop(1, CLUSTERS, start_second_rest, 0)
        table[my_half, my_group, PARTS - 1] = picked[me, PARTS - 1]

    lax.fori_loop(4, steps, prepare, 0)

    pltpu.make_async_copy(others, others, send_a).wait()
    sent = picked.at[pl.ds(0, CLUSTERS - 1), pl.ds(0, PARTS - 1)]
    tail = picked.at[pl.ds(0, CLUSTERS - 1), pl.ds(PARTS - 1, 1)]
    pltpu.make_async_copy(sent, sent, send_c).wait()

    @pl.when(my_group < FULL)
    def _():
        fewer = slices.at[pl.ds(0, 2 * FULL - 1), pl.ds(PARTS - 1, 1)]
        pltpu.make_async_copy(fewer, fewer, send_b).wait()
        pltpu.make_async_copy(tail, tail, send_d).wait()
        less = picked.at[pl.ds(0, 2 * FULL - 1), pl.ds(PARTS - 1, 1)]
        pltpu.make_async_copy(less, less, recv_d).wait()

    @pl.when(my_group >= FULL)
    def _():
        fewer = slices.at[pl.ds(0, 2 * FULL), pl.ds(PARTS - 1, 1)]
        pltpu.make_async_copy(fewer, fewer, send_b).wait()
        less = picked.at[pl.ds(0, 2 * FULL), pl.ds(PARTS - 1, 1)]
        pltpu.make_async_copy(less, less, recv_d).wait()

    pltpu.make_async_copy(sent, sent, recv_c).wait()
    for i in range(PARTS):
        both = jnp.concatenate([table[h, :, i].reshape(KG * SLOTS, HALF) for h in range(2)], axis=1)
        turned = jnp.dot(turn[...], both, preferred_element_type=F32).astype(BF16)
        matrix[:, i * KG : (i + 1) * KG, :] = turned.reshape(SLOTS, KG, DIRS)

    def exchange(t):
        way = (1 - 2 * lax.rem(t, 2)) * (1 - 2 * lax.rem(lax.div(t, 2), 2))
        return pltpu.make_async_remote_copy(
            src_ref=parts.at[t],
            dst_ref=got.at[t],
            send_sem=send_sem.at[t],
            recv_sem=recv_sem.at[t],
            device_id={"dir": lax.rem(row + way + 4, 4)},
            device_id_type=MESH,
        )

    def step(t, carry):
        base = lax.div(first_of(t), HALF)
        for n in range(NB // NI):
            cols = slice(n * NI, (n + 1) * NI)
            held, code = weight[t, :, cols], slot[t, :, cols]
            bounce = None
            for s in range(SLOTS):
                spread = jnp.where(code == jnp.int16(s), held, jnp.zeros_like(held))
                term = jnp.dot(matrix[s], spread, preferred_element_type=F32)
                bounce = term if bounce is None else bounce + term
            gain = SCALE * across(albedo_ref, base + n * (NI // HALF))
            total[:, cols] = direct[t, :, cols] + gain * bounce

        @pl.when(t < 4)
        def _():
            parts[t] = total[:SEND].astype(BF16)
            exchange(t).start()

        @pl.when(lax.div(t, 2) == 2)
        def _():
            exchange(t - 4).wait_recv()
            parts[t] = (total[:SEND] + got[t - 4].astype(F32)).astype(BF16)
            exchange(t).start()

        @pl.when(t >= 6)
        def _():
            exchange(t - 4).wait_recv()
            exchange(t - 2).wait_recv()
            mine = total[:SEND] + got[t - 4].astype(F32) + got[t - 2].astype(F32)
            out_ref[:, pl.ds(pl.multiple_of((t - 6) * NB, NB), NB)] = mine[:COEFFS].astype(BF16)

        return carry

    lax.fori_loop(0, steps, step, 0)
    for t in range(steps - 2):
        exchange(t).wait_send()


def per_device(
    ray_code, occluder_list, list_count, normal_azimuth, normal_height, albedo, occluder_exit_radiance
):
    harmonics, axes = direction_tables()
    high = harmonics.astype(BF16)
    harmonics = np.concatenate([high, (harmonics - high.astype(np.float32)).astype(BF16)], axis=1)
    blocks = jnp.pad(occluder_exit_radiance, ((0, 0), (0, ROWS - COEFFS), (0, 0)))
    blocks = blocks.reshape(BLK, PARTS, KG, 2, HALF).transpose(3, 2, 1, 0, 4)
    vmem = pl.BlockSpec(memory_space=pltpu.VMEM)
    steps = VERTS // NB
    by_lane = (VERTS // HALF, HALF)
    dma = pltpu.SemaphoreType.DMA
    return pl.pallas_call(
        transfer_kernel,
        out_shape=jax.ShapeDtypeStruct((COEFFS, OWN), BF16),
        in_specs=[
            pl.BlockSpec(memory_space=pl.ANY),
            pl.BlockSpec(memory_space=pltpu.SMEM),
        ]
        + [vmem] * 7,
        out_specs=vmem,
        scratch_shapes=[
            pltpu.VMEM((steps, DIRS, NB), jnp.int32),
            pltpu.VMEM((steps, DIRS, NB), BF16),
            pltpu.VMEM((steps, DIRS, NB), jnp.int16),
            pltpu.VMEM((steps, ROWS, NB), F32),
            pltpu.VMEM((ROWS, NB), F32),
            pltpu.VMEM((2,) + by_lane, F32),
            pltpu.VMEM((CLUSTERS * SLOTS, CLUSTERS * BLK), BF16),
            pltpu.VMEM((SLOTS * KG, SLOTS * KG), BF16),
            pltpu.VMEM((CLUSTERS, PARTS, BLK, HALF), BF16),
            pltpu.VMEM((CLUSTERS, PARTS, SLOTS, HALF), BF16),
            pltpu.VMEM((2, KG, PARTS, SLOTS, HALF), BF16),
            pltpu.VMEM((SLOTS, ROWS, DIRS), BF16),
            pltpu.VMEM((steps - 2, SEND, NB), BF16),
            pltpu.VMEM((steps - 2, SEND, NB), BF16),
            dma((steps,)),
        ]
        + [dma] * 8
        + [dma((steps - 2,)), dma((steps - 2,))],
        compiler_params=pltpu.CompilerParams(
            collective_id=0, has_side_effects=True, vmem_limit_bytes=60 << 20
        ),
        name="transfer",
    )(
        ray_code,
        list_count,
        blocks,
        occluder_list.reshape(CLUSTERS * SLOTS, 1),
        jnp.asarray(axes),
        normal_azimuth.reshape(by_lane),
        normal_height.reshape(by_lane),
        albedo.reshape(by_lane),
        jnp.asarray(harmonics),
    )


def solution(mesh):
    return jax.shard_map(
        per_device,
        mesh=mesh,
        in_specs=(
            P("dir", "cluster"),
            P(),
            P(),
            P("cluster"),
            P("cluster"),
            P("cluster"),
            P("cluster", None, "dir"),
        ),
        out_specs=P(None, ("cluster", "dir")),
        check_vma=False,
    )
```

```python
import math

import jax
import jax.numpy as jnp
import numpy as np
from jax import lax
from jax.experimental import pallas as pl
from jax.experimental.pallas import tpu as pltpu
from jax.sharding import PartitionSpec as P

NDIR = 1024
SHORD = 9
COEFFS = 81
SLOTS = 16
CLUSTERS = 64
BLK = 8
DIRS = 256
HALF = 128
VERTS = 8192
OWN = 2048
KG = 32
PARTS = 3
ROWS = KG * PARTS
SEND = 88
FULL = COEFFS - KG * (PARTS - 1)
NB = 512
NI = 256
F32 = jnp.float32
BF16 = jnp.bfloat16
MESH = pl.DeviceIdType.MESH
SCALE = 4.0 * math.pi / NDIR
GOLDEN = math.pi * (3.0 - math.sqrt(5.0))


def direction_tables():
    p = np.arange(NDIR, dtype=np.float32)
    z = (np.float32(1.0) - (np.float32(2.0) * p + np.float32(1.0)) / np.float32(NDIR)).astype(np.float32)
    r = np.sqrt(np.maximum(np.float32(1.0) - z * z, np.float32(0.0)))
    t = (p * np.float32(GOLDEN)).astype(np.float64)
    x = (r * np.cos(t).astype(np.float32)).astype(np.float64)
    y = (r * np.sin(t).astype(np.float32)).astype(np.float64)
    z = z.astype(np.float64)
    c, s = [np.ones_like(x)], [np.zeros_like(x)]
    for _ in range(1, SHORD):
        c.append(c[-1] * x - s[-1] * y)
        s.append(c[-2] * y + s[-1] * x)
    rows = [None] * COEFFS
    for m in range(SHORD):
        q = [None] * SHORD
        q[m] = np.full_like(z, float(np.prod(np.arange(1, 2 * m, 2, dtype=np.float64))))
        if m + 1 < SHORD:
            q[m + 1] = z * (2 * m + 1) * q[m]
        for l in range(m + 2, SHORD):
            q[l] = ((2 * l - 1) * z * q[l - 1] - (l + m - 1) * q[l - 2]) / (l - m)
        for l in range(m, SHORD):
            n = math.sqrt((2 * l + 1) / (4.0 * math.pi) * math.factorial(l - m) / math.factorial(l + m))
            at = l * l + l
            if m == 0:
                rows[at] = n * q[l]
            else:
                rows[at + m] = math.sqrt(2.0) * n * q[l] * c[m]
                rows[at - m] = math.sqrt(2.0) * n * q[l] * s[m]
    table = np.zeros((4, ROWS, DIRS), np.float32)
    table[:, :COEFFS] = np.stack(rows).reshape(COEFFS, 4, DIRS).transpose(1, 0, 2)
    axes = np.zeros((4, DIRS, 8), np.float32)
    for i, a in enumerate((x, y, z)):
        axes[:, :, i] = a.reshape(4, DIRS)
    return table, axes


def place(x, z, core):
    return core, lax.rem((z * 4 + x) * 5, KG)


def transfer_kernel(
    code_ref, count_ref, block_hbm, list_hbm, axes_hbm, azimuth_hbm, height_hbm, albedo_hbm, harm_hbm, out_ref,
    list_ref, axes_ref, azimuth_ref, height_ref, albedo_ref, harm_ref, codes, weight, slot, direct, total, own, normal, chosen, turn, blocks, slices, picked, table, matrix, parts, got,
    load_sem, code_sem, send_a, recv_a, send_b, recv_b, send_sem, recv_sem,
):
    me = lax.axis_index("cluster")
    row = lax.axis_index("dir")
    my_x, my_z, my_core = lax.div(me, 16), lax.rem(lax.div(me, 2), 8), lax.rem(me, 2)
    my_half, my_group = place(my_x, my_z, my_core)
    steps = VERTS // NB
    subs = OWN // NB

    def peer_of(i):
        j, r = lax.div(i, 8), lax.rem(i, 8)
        m = lax.div(r, 2)
        z = lax.rem(my_z + 4 + lax.div(j + 1, 2) * (1 - 2 * lax.rem(j, 2)), 8)
        x = lax.rem(my_x + 2 + lax.div(m + 1, 2) * (1 - 2 * lax.rem(m, 2)), 4)
        core = lax.rem(my_core + 1 + r, 2)
        return x, z, core

    def at(x, z, core):
        return {"cluster": x * 16 + z * 2 + core}

    def first_of(t):
        pair, half = lax.div(t, subs), lax.rem(t, 2)
        ahead = lax.rem(2 + pair, 4) + lax.div(pair, 2) * (1 - 2 * lax.rem(pair, 2))
        ahead = ahead + 2 * half * lax.rem(lax.div(pair + 1, 2), 2)
        inner = half * (subs // 2) + lax.rem(lax.div(t, 2), subs // 2)
        return pl.multiple_of(lax.rem(row + ahead, 4) * OWN + inner * NB, NB)

    def fetch(t):
        return pltpu.make_async_copy(code_ref.at[:, pl.ds(first_of(t), NB)], codes.at[t], code_sem.at[t])

    loads = [
        pltpu.make_async_copy(source, target, load_sem.at[i])
        for i, (source, target) in enumerate(
            (
                (block_hbm, blocks),
                (list_hbm, list_ref),
                (azimuth_hbm, azimuth_ref),
                (height_hbm, height_ref),
                (albedo_hbm, albedo_ref),
                (axes_hbm.at[row], axes_ref),
                (harm_hbm.at[row], harm_ref),
            )
        )
    ]
    barrier = pltpu.get_barrier_semaphore()

    def greet(i, carry):
        pl.semaphore_signal(barrier, inc=1, device_id=at(*peer_of(i)), device_id_type=MESH)
        return carry

    lax.fori_loop(0, CLUSTERS - 1, greet, 0)
    for i in (1, 3):
        pl.semaphore_signal(barrier, inc=1, device_id={"dir": lax.rem(row + i, 4)}, device_id_type=MESH)

    for load in loads:
        load.start()

    def start_fetch(t, carry):
        fetch(t).start()
        return carry

    lax.fori_loop(0, steps, start_fetch, 0)

    for load in loads:
        load.wait()
    my_lanes = pl.ds(pl.multiple_of(my_half * HALF, HALF), HALF)
    for unit in range(PARTS - 1):
        slices[me, unit] = blocks[unit * KG + my_group, :, my_lanes]

    @pl.when(my_group < FULL)
    def _():
        slices[me, PARTS - 1] = blocks[(PARTS - 1) * KG + my_group, :, my_lanes]

    lists = jnp.broadcast_to(list_ref[...].astype(F32).T[:, None, :], (CLUSTERS, SLOTS, SLOTS))
    here = lax.broadcasted_iota(jnp.int32, lists.shape, 1) == lax.broadcasted_iota(jnp.int32, lists.shape, 2)
    column = jnp.sum(jnp.where(here, lists, 0.0), axis=2, keepdims=True).reshape(CLUSTERS * SLOTS, 1)
    each = lax.broadcasted_iota(jnp.int32, (CLUSTERS * SLOTS, CLUSTERS * BLK), 1).astype(F32)
    chosen[...] = jnp.where(column == each, 1.0, 0.0).astype(BF16)
    to = lax.broadcasted_iota(jnp.int32, (SLOTS * KG, SLOTS * KG), 0)
    fro = lax.broadcasted_iota(jnp.int32, (SLOTS * KG, SLOTS * KG), 1)
    turn[...] = jnp.where((to % KG) * SLOTS + to // KG == fro, 1.0, 0.0).astype(BF16)
    table[:, FULL:, PARTS - 1] = jnp.zeros((2, KG - FULL, SLOTS, HALF), BF16)
    height = height_ref[...]
    planar = jnp.sqrt(jnp.maximum(1.0 - height * height, 0.0))
    normal[0] = planar * jnp.cos(azimuth_ref[...])
    normal[1] = planar * jnp.sin(azimuth_ref[...])
    pl.semaphore_wait(barrier, CLUSTERS + 1)

    def first(peer, unit):
        half, group = place(*peer)
        return pltpu.make_async_remote_copy(
            src_ref=blocks.at[unit * KG + group, :, pl.ds(pl.multiple_of(half * HALF, HALF), HALF)],
            dst_ref=slices.at[me, unit],
            send_sem=send_a.at[unit],
            recv_sem=recv_a.at[unit],
            device_id=at(*peer),
            device_id_type=MESH,
        )

    def start_first(i, carry):
        first(peer_of(i), 0).start()
        return carry

    def start_first_rest(i, carry):
        peer = peer_of(i)
        first(peer, 1).start()

        @pl.when(place(*peer)[1] < FULL)
        def _():
            first(peer, 2).start()

        return carry

    lax.fori_loop(0, CLUSTERS - 1, start_first, 0)
    lax.fori_loop(0, CLUSTERS - 1, start_first_rest, 0)

    count = count_ref[me]
    x, y, z = (axes_ref[:, i : i + 1] for i in range(3))

    def across(ref, at):
        return jnp.concatenate([ref[pl.ds(at + i, 1), :] for i in range(NI // HALF)], axis=1)

    def prepare(t, carry):
        fetch(t).wait()
        base = lax.div(first_of(t), HALF)
        for n in range(NB // NI):
            cols = slice(n * NI, (n + 1) * NI)
            at = base + n * (NI // HALF)
            code = codes[t, :, cols]
            facing = jnp.maximum(
                x * across(normal.at[0], at) + y * across(normal.at[1], at) + z * across(height_ref, at), 0.0
            )
            hit = code < count
            weight[t, :, cols] = facing.astype(BF16)
            slot[t, :, cols] = jnp.where(hit, code, SLOTS).astype(jnp.int16)
            lit = jnp.where(hit, 0.0, facing)
            high = lit.astype(BF16)
            low = (lit - high.astype(F32)).astype(BF16)
            both = jnp.dot(harm_ref[...], high, preferred_element_type=F32)
            rest = jnp.dot(harm_ref[:ROWS], low, preferred_element_type=F32)
            direct[t, :, cols] = SCALE * (both[:ROWS] + both[ROWS:] + rest)
        return carry

    def choose(unit):
        others = slices.at[pl.ds(0, CLUSTERS - 1), unit]
        pltpu.make_async_copy(others, others, recv_a.at[unit]).wait()
        held = slices[:, unit].reshape(CLUSTERS * BLK, HALF)
        rows = jnp.dot(chosen[...], held, preferred_element_type=F32).astype(BF16)
        picked[:, unit] = rows.reshape(CLUSTERS, SLOTS, HALF)

    def second(i, unit):
        peer = peer_of(i)
        return pltpu.make_async_remote_copy(
            src_ref=picked.at[at_index(peer), unit],
            dst_ref=table.at[my_half, my_group, unit],
            send_sem=send_b.at[unit],
            recv_sem=recv_b.at[unit],
            device_id=at(*peer),
            device_id_type=MESH,
        )

    def at_index(peer):
        return peer[0] * 16 + peer[1] * 2 + peer[2]

    def start_second(unit):
        def body(i, carry):
            second(i, unit).start()
            return carry

        return body

    lax.fori_loop(0, 6, prepare, 0)
    choose(0)
    lax.fori_loop(0, CLUSTERS - 1, start_second(0), 0)
    lax.fori_loop(6, 8, prepare, 0)
    choose(1)
    lax.fori_loop(0, CLUSTERS - 1, start_second(1), 0)

    @pl.when(my_group < FULL)
    def _():
        choose(2)
        lax.fori_loop(0, CLUSTERS - 1, start_second(2), 0)
        table[my_half, my_group, 2] = picked[me, 2]

    for unit in range(PARTS - 1):
        table[my_half, my_group, unit] = picked[me, unit]

    lax.fori_loop(8, steps, prepare, 0)

    for unit in range(PARTS - 1):
        others = slices.at[pl.ds(0, CLUSTERS - 1), unit]
        sent = picked.at[pl.ds(0, CLUSTERS - 1), unit]
        pltpu.make_async_copy(others, others, send_a.at[unit]).wait()
        pltpu.make_async_copy(sent, sent, send_b.at[unit]).wait()

    def spread_part(i):
        both = jnp.concatenate([table[h, :, i].reshape(KG * SLOTS, HALF) for h in range(2)], axis=1)
        turned = jnp.dot(turn[...], both, preferred_element_type=F32).astype(BF16)
        matrix[:, i * KG : (i + 1) * KG, :] = turned.reshape(SLOTS, KG, DIRS)

    for unit in range(PARTS - 1):
        sent = picked.at[pl.ds(0, CLUSTERS - 1), unit]
        pltpu.make_async_copy(sent, sent, recv_b.at[unit]).wait()
        spread_part(unit)

    @pl.when(my_group < FULL)
    def _():
        fewer = slices.at[pl.ds(0, 2 * FULL - 1), 2]
        pltpu.make_async_copy(fewer, fewer, send_a.at[2]).wait()
        tail = picked.at[pl.ds(0, CLUSTERS - 1), 2]
        pltpu.make_async_copy(tail, tail, send_b.at[2]).wait()
        less = picked.at[pl.ds(0, 2 * FULL - 1), 2]
        pltpu.make_async_copy(less, less, recv_b.at[2]).wait()

    @pl.when(my_group >= FULL)
    def _():
        fewer = slices.at[pl.ds(0, 2 * FULL), 2]
        pltpu.make_async_copy(fewer, fewer, send_a.at[2]).wait()
        less = picked.at[pl.ds(0, 2 * FULL), 2]
        pltpu.make_async_copy(less, less, recv_b.at[2]).wait()

    spread_part(2)

    def exchange(t):
        way = (1 - 2 * lax.rem(t, 2)) * (1 - 2 * lax.rem(lax.div(t, subs), 2))
        return pltpu.make_async_remote_copy(
            src_ref=parts.at[t],
            dst_ref=got.at[t],
            send_sem=send_sem.at[t],
            recv_sem=recv_sem.at[t],
            device_id={"dir": lax.rem(row + way + 4, 4)},
            device_id_type=MESH,
        )

    wide = NB // HALF

    def pack(t, sums):
        for r in range(COEFFS // 8):
            for c in range(wide):
                parts[t, r * wide + c] = sums[r * 8 : r * 8 + 8, c * HALF : (c + 1) * HALF].astype(BF16)
        end = [sums[COEFFS - 1 : COEFFS, c * HALF : (c + 1) * HALF] for c in range(wide)]
        parts[t, COEFFS // 8 * wide] = jnp.concatenate(end * (8 // wide), axis=0).astype(BF16)

    def unpack(t):
        tiles = [got[t, i].astype(F32) for i in range(COEFFS // 8 * wide + 1)]
        rows = [jnp.concatenate(tiles[r * wide : (r + 1) * wide], axis=1) for r in range(COEFFS // 8)]
        end = jnp.concatenate([tiles[-1][c : c + 1] for c in range(wide)], axis=1)
        return jnp.concatenate(rows + [jnp.broadcast_to(end, (8, NB))], axis=0)

    def step(t, carry):
        base = lax.div(first_of(t), HALF)
        for n in range(NB // NI):
            cols = slice(n * NI, (n + 1) * NI)
            held, code = weight[t, :, cols], slot[t, :, cols]
            bounce = None
            for s in range(SLOTS):
                spread = jnp.where(code == jnp.int16(s), held, jnp.zeros_like(held))
                term = jnp.dot(matrix[s], spread, preferred_element_type=F32)
                bounce = term if bounce is None else bounce + term
            gain = SCALE * across(albedo_ref, base + n * (NI // HALF))
            total[:, cols] = direct[t, :, cols] + gain * bounce

        @pl.when(t < 2 * subs)
        def _():
            pack(t, total[:SEND])
            exchange(t).start()

        @pl.when(lax.div(t, subs) == 2)
        def _():
            exchange(t - 2 * subs).wait_recv()
            pack(t, total[:SEND] + unpack(t - 2 * subs))
            exchange(t).start()

        @pl.when(t >= 3 * subs)
        def _():
            own[t - 3 * subs] = total[:SEND]

        return carry

    lax.fori_loop(0, steps, step, 0)
    for i in range(subs):
        exchange(subs + i).wait_recv()
        exchange(2 * subs + i).wait_recv()
        mine = own[i] + unpack(subs + i) + unpack(2 * subs + i)
        begin = ((i % 2) * (subs // 2) + i // 2) * NB
        out_ref[:, begin : begin + NB] = mine[:COEFFS].astype(BF16)
    for t in range(3 * subs):
        exchange(t).wait_send()


def per_device(
    ray_code, occluder_list, list_count, normal_azimuth, normal_height, albedo, occluder_exit_radiance
):
    harmonics, axes = direction_tables()
    high = harmonics.astype(BF16)
    harmonics = np.concatenate([high, (harmonics - high.astype(np.float32)).astype(BF16)], axis=1)
    hbm = pl.BlockSpec(memory_space=pltpu.HBM)
    tiles = COEFFS // 8 * (NB // HALF) + 1
    steps = VERTS // NB
    sends = 3 * (OWN // NB)
    by_lane = (VERTS // HALF, HALF)
    dma = pltpu.SemaphoreType.DMA
    return pl.pallas_call(
        transfer_kernel,
        out_shape=jax.ShapeDtypeStruct((COEFFS, OWN), BF16),
        in_specs=[hbm, pl.BlockSpec(memory_space=pltpu.SMEM)] + [hbm] * 7,
        out_specs=pl.BlockSpec(memory_space=pltpu.VMEM),
        scratch_shapes=[
            pltpu.VMEM((SLOTS, CLUSTERS), jnp.int32),
            pltpu.VMEM((DIRS, 8), F32),
            pltpu.VMEM(by_lane, F32),
            pltpu.VMEM(by_lane, F32),
            pltpu.VMEM(by_lane, F32),
            pltpu.VMEM((2 * ROWS, DIRS), BF16),
            pltpu.VMEM((steps, DIRS, NB), jnp.int32),
            pltpu.VMEM((steps, DIRS, NB), BF16),
            pltpu.VMEM((steps, DIRS, NB), jnp.int16),
            pltpu.VMEM((steps, ROWS, NB), F32),
            pltpu.VMEM((ROWS, NB), F32),
            pltpu.VMEM((OWN // NB, SEND, NB), F32),
            pltpu.VMEM((2,) + by_lane, F32),
            pltpu.VMEM((CLUSTERS * SLOTS, CLUSTERS * BLK), BF16),
            pltpu.VMEM((SLOTS * KG, SLOTS * KG), BF16),
            pltpu.VMEM((COEFFS, BLK, DIRS), BF16),
            pltpu.VMEM((CLUSTERS, PARTS, BLK, HALF), BF16),
            pltpu.VMEM((CLUSTERS, PARTS, SLOTS, HALF), BF16),
            pltpu.VMEM((2, KG, PARTS, SLOTS, HALF), BF16),
            pltpu.VMEM((SLOTS, ROWS, DIRS), BF16),
            pltpu.VMEM((sends, tiles, 8, HALF), BF16),
            pltpu.VMEM((sends, tiles, 8, HALF), BF16),
            dma((7,)),
            dma((steps,)),
        ]
        + [dma((PARTS,))] * 4
        + [dma((sends,)), dma((sends,))],
        compiler_params=pltpu.CompilerParams(
            collective_id=0, has_side_effects=True, vmem_limit_bytes=60 << 20
        ),
        name="transfer",
    )(
        ray_code,
        list_count,
        occluder_exit_radiance.transpose(1, 0, 2),
        occluder_list.T,
        jnp.asarray(axes),
        normal_azimuth.reshape(by_lane),
        normal_height.reshape(by_lane),
        albedo.reshape(by_lane),
        jnp.asarray(harmonics),
    )


def solution(mesh):
    return jax.shard_map(
        per_device,
        mesh=mesh,
        in_specs=(
            P("dir", "cluster"),
            P(),
            P(),
            P("cluster"),
            P("cluster"),
            P("cluster"),
            P("cluster", None, "dir"),
        ),
        out_specs=P(None, ("cluster", "dir")),
        check_vma=False,
    )
```

```python
import math

import jax
import jax.numpy as jnp
import numpy as np
from jax import lax
from jax.experimental import pallas as pl
from jax.experimental.pallas import tpu as pltpu
from jax.sharding import PartitionSpec as P

NDIR = 1024
SHORD = 9
COEFFS = 81
SLOTS = 16
CLUSTERS = 64
BLK = 8
DIRS = 256
HALF = 128
VERTS = 8192
OWN = 2048
KG = 32
PARTS = 3
ROWS = KG * PARTS
SEND = 88
FULL = COEFFS - KG * (PARTS - 1)
NB = 512
NI = 256
F32 = jnp.float32
BF16 = jnp.bfloat16
MESH = pl.DeviceIdType.MESH
SCALE = 4.0 * math.pi / NDIR
GOLDEN = math.pi * (3.0 - math.sqrt(5.0))


def direction_tables():
    p = np.arange(NDIR, dtype=np.float32)
    z = (np.float32(1.0) - (np.float32(2.0) * p + np.float32(1.0)) / np.float32(NDIR)).astype(np.float32)
    r = np.sqrt(np.maximum(np.float32(1.0) - z * z, np.float32(0.0)))
    t = (p * np.float32(GOLDEN)).astype(np.float64)
    x = (r * np.cos(t).astype(np.float32)).astype(np.float64)
    y = (r * np.sin(t).astype(np.float32)).astype(np.float64)
    z = z.astype(np.float64)
    c, s = [np.ones_like(x)], [np.zeros_like(x)]
    for _ in range(1, SHORD):
        c.append(c[-1] * x - s[-1] * y)
        s.append(c[-2] * y + s[-1] * x)
    rows = [None] * COEFFS
    for m in range(SHORD):
        q = [None] * SHORD
        q[m] = np.full_like(z, float(np.prod(np.arange(1, 2 * m, 2, dtype=np.float64))))
        if m + 1 < SHORD:
            q[m + 1] = z * (2 * m + 1) * q[m]
        for l in range(m + 2, SHORD):
            q[l] = ((2 * l - 1) * z * q[l - 1] - (l + m - 1) * q[l - 2]) / (l - m)
        for l in range(m, SHORD):
            n = math.sqrt((2 * l + 1) / (4.0 * math.pi) * math.factorial(l - m) / math.factorial(l + m))
            at = l * l + l
            if m == 0:
                rows[at] = n * q[l]
            else:
                rows[at + m] = math.sqrt(2.0) * n * q[l] * c[m]
                rows[at - m] = math.sqrt(2.0) * n * q[l] * s[m]
    table = np.zeros((4, ROWS, DIRS), np.float32)
    table[:, :COEFFS] = np.stack(rows).reshape(COEFFS, 4, DIRS).transpose(1, 0, 2)
    axes = np.zeros((4, DIRS, 8), np.float32)
    for i, a in enumerate((x, y, z)):
        axes[:, :, i] = a.reshape(4, DIRS)
    return table, axes


def place(x, z, core):
    return core, lax.rem((z * 4 + x) * 5, KG)


def transfer_kernel(
    code_ref, count_hbm, block_hbm, list_hbm, axes_hbm, azimuth_hbm, height_hbm, albedo_hbm, harm_hbm, out_ref,
    count_ref, list_ref, axes_ref, azimuth_ref, height_ref, albedo_ref, harm_ref, codes, weight, slot, direct, total, own, normal, chosen, turn, blocks, slices, picked, table, matrix, parts, got,
    load_sem, code_sem, send_a, recv_a, send_b, recv_b, send_sem, recv_sem,
):
    me = lax.axis_index("cluster")
    row = lax.axis_index("dir")
    my_x, my_z, my_core = lax.div(me, 16), lax.rem(lax.div(me, 2), 8), lax.rem(me, 2)
    my_half, my_group = place(my_x, my_z, my_core)
    steps = VERTS // NB
    subs = OWN // NB

    columns = [lax.rem(my_x + i, 4) for i in range(4)]
    cores = [my_core, 1 - my_core]

    def each_peer(act):
        def visit(j, carry):
            z = lax.rem(my_z + 4 + lax.div(j + 1, 2) * (1 - 2 * lax.rem(j, 2)), 8)
            for dx in (2, 1, 3, 0):
                for flip in (1, 0):
                    if dx or flip:
                        act((columns[dx], z, cores[flip]))
                    else:

                        @pl.when(j < 7)
                        def _():
                            act((columns[0], z, cores[0]))

            return carry

        lax.fori_loop(0, 8, visit, 0)

    def at(x, z, core):
        return {"cluster": x * 16 + z * 2 + core}

    def first_of(t):
        pair, half = lax.div(t, subs), lax.rem(t, 2)
        ahead = lax.rem(2 + pair, 4) + lax.div(pair, 2) * (1 - 2 * lax.rem(pair, 2))
        ahead = ahead + 2 * half * lax.rem(lax.div(pair + 1, 2), 2)
        inner = half * (subs // 2) + lax.rem(lax.div(t, 2), subs // 2)
        return pl.multiple_of(lax.rem(row + ahead, 4) * OWN + inner * NB, NB)

    def fetch(t):
        return pltpu.make_async_copy(code_ref.at[:, pl.ds(first_of(t), NB)], codes.at[t], code_sem.at[t])

    loads = [
        pltpu.make_async_copy(source, target, load_sem.at[i])
        for i, (source, target) in enumerate(
            (
                (block_hbm, blocks),
                (count_hbm, count_ref),
                (list_hbm, list_ref),
                (azimuth_hbm, azimuth_ref),
                (height_hbm, height_ref),
                (albedo_hbm, albedo_ref),
                (axes_hbm.at[row], axes_ref),
                (harm_hbm.at[row], harm_ref),
            )
        )
    ]
    barrier = pltpu.get_barrier_semaphore()

    def greet(peer):
        pl.semaphore_signal(barrier, inc=1, device_id=at(*peer), device_id_type=MESH)

    each_peer(greet)
    for i in (1, 3):
        pl.semaphore_signal(barrier, inc=1, device_id={"dir": lax.rem(row + i, 4)}, device_id_type=MESH)

    for load in loads:
        load.start()

    def start_fetch(t, carry):
        fetch(t).start()
        return carry

    lax.fori_loop(0, steps, start_fetch, 0)

    for load in loads:
        load.wait()
    my_lanes = pl.ds(pl.multiple_of(my_half * HALF, HALF), HALF)
    for unit in range(PARTS - 1):
        slices[me, unit] = blocks[unit * KG + my_group, :, my_lanes]

    @pl.when(my_group < FULL)
    def _():
        slices[me, PARTS - 1] = blocks[(PARTS - 1) * KG + my_group, :, my_lanes]

    lists = jnp.broadcast_to(list_ref[...].astype(F32).T[:, None, :], (CLUSTERS, SLOTS, SLOTS))
    here = lax.broadcasted_iota(jnp.int32, lists.shape, 1) == lax.broadcasted_iota(jnp.int32, lists.shape, 2)
    column = jnp.sum(jnp.where(here, lists, 0.0), axis=2, keepdims=True).reshape(CLUSTERS * SLOTS, 1)
    each = lax.broadcasted_iota(jnp.int32, (CLUSTERS * SLOTS, CLUSTERS * BLK), 1).astype(F32)
    chosen[...] = jnp.where(column == each, 1.0, 0.0).astype(BF16)
    to = lax.broadcasted_iota(jnp.int32, (SLOTS * KG, SLOTS * KG), 0)
    fro = lax.broadcasted_iota(jnp.int32, (SLOTS * KG, SLOTS * KG), 1)
    turn[...] = jnp.where((to % KG) * SLOTS + to // KG == fro, 1.0, 0.0).astype(BF16)
    table[:, FULL:, PARTS - 1] = jnp.zeros((2, KG - FULL, SLOTS, HALF), BF16)
    height = height_ref[...]
    planar = jnp.sqrt(jnp.maximum(1.0 - height * height, 0.0))
    normal[0] = planar * jnp.cos(azimuth_ref[...])
    normal[1] = planar * jnp.sin(azimuth_ref[...])
    pl.semaphore_wait(barrier, CLUSTERS + 1)

    def first(peer, unit):
        half, group = place(*peer)
        return pltpu.make_async_remote_copy(
            src_ref=blocks.at[unit * KG + group, :, pl.ds(pl.multiple_of(half * HALF, HALF), HALF)],
            dst_ref=slices.at[me, unit],
            send_sem=send_a.at[unit],
            recv_sem=recv_a.at[unit],
            device_id=at(*peer),
            device_id_type=MESH,
        )

    def start_first(peer):
        first(peer, 0).start()

    def start_first_rest(peer):
        first(peer, 1).start()

        @pl.when(place(*peer)[1] < FULL)
        def _():
            first(peer, 2).start()

    each_peer(start_first)
    each_peer(start_first_rest)

    count = count_ref[me]
    x, y, z = (axes_ref[:, i : i + 1] for i in range(3))

    def across(ref, at):
        return jnp.concatenate([ref[pl.ds(at + i, 1), :] for i in range(NI // HALF)], axis=1)

    def prepare(t, carry):
        fetch(t).wait()
        base = lax.div(first_of(t), HALF)
        for n in range(NB // NI):
            cols = slice(n * NI, (n + 1) * NI)
            at = base + n * (NI // HALF)
            code = codes[t, :, cols]
            facing = jnp.maximum(
                x * across(normal.at[0], at) + y * across(normal.at[1], at) + z * across(height_ref, at), 0.0
            )
            hit = code < count
            weight[t, :, cols] = facing.astype(BF16)
            slot[t, :, cols] = jnp.where(hit, code, SLOTS).astype(jnp.int16)
            lit = jnp.where(hit, 0.0, facing)
            high = lit.astype(BF16)
            low = (lit - high.astype(F32)).astype(BF16)
            both = jnp.dot(harm_ref[...], high, preferred_element_type=F32)
            rest = jnp.dot(harm_ref[:ROWS], low, preferred_element_type=F32)
            direct[t, :, cols] = SCALE * (both[:ROWS] + both[ROWS:] + rest)
        return carry

    def choose(unit):
        others = slices.at[pl.ds(0, CLUSTERS - 1), unit]
        pltpu.make_async_copy(others, others, recv_a.at[unit]).wait()
        held = slices[:, unit].reshape(CLUSTERS * BLK, HALF)
        rows = jnp.dot(chosen[...], held, preferred_element_type=F32).astype(BF16)
        picked[:, unit] = rows.reshape(CLUSTERS, SLOTS, HALF)

    def second(unit):
        def start(peer):
            pltpu.make_async_remote_copy(
                src_ref=picked.at[at(*peer)["cluster"], unit],
                dst_ref=table.at[my_half, my_group, unit],
                send_sem=send_b.at[unit],
                recv_sem=recv_b.at[unit],
                device_id=at(*peer),
                device_id_type=MESH,
            ).start()

        each_peer(start)

    lax.fori_loop(0, 4, prepare, 0)
    choose(0)
    second(0)
    lax.fori_loop(4, 8, prepare, 0)
    choose(1)
    second(1)

    @pl.when(my_group < FULL)
    def _():
        choose(2)
        second(2)
        table[my_half, my_group, 2] = picked[me, 2]

    for unit in range(PARTS - 1):
        table[my_half, my_group, unit] = picked[me, unit]

    lax.fori_loop(8, steps, prepare, 0)

    for unit in range(PARTS - 1):
        others = slices.at[pl.ds(0, CLUSTERS - 1), unit]
        sent = picked.at[pl.ds(0, CLUSTERS - 1), unit]
        pltpu.make_async_copy(others, others, send_a.at[unit]).wait()
        pltpu.make_async_copy(sent, sent, send_b.at[unit]).wait()

    def spread_part(i):
        both = jnp.concatenate([table[h, :, i].reshape(KG * SLOTS, HALF) for h in range(2)], axis=1)
        turned = jnp.dot(turn[...], both, preferred_element_type=F32).astype(BF16)
        matrix[:, i * KG : (i + 1) * KG, :] = turned.reshape(SLOTS, KG, DIRS)

    for unit in range(PARTS - 1):
        sent = picked.at[pl.ds(0, CLUSTERS - 1), unit]
        pltpu.make_async_copy(sent, sent, recv_b.at[unit]).wait()
        spread_part(unit)

    @pl.when(my_group < FULL)
    def _():
        fewer = slices.at[pl.ds(0, 2 * FULL - 1), 2]
        pltpu.make_async_copy(fewer, fewer, send_a.at[2]).wait()
        tail = picked.at[pl.ds(0, CLUSTERS - 1), 2]
        pltpu.make_async_copy(tail, tail, send_b.at[2]).wait()
        less = picked.at[pl.ds(0, 2 * FULL - 1), 2]
        pltpu.make_async_copy(less, less, recv_b.at[2]).wait()

    @pl.when(my_group >= FULL)
    def _():
        fewer = slices.at[pl.ds(0, 2 * FULL), 2]
        pltpu.make_async_copy(fewer, fewer, send_a.at[2]).wait()
        less = picked.at[pl.ds(0, 2 * FULL), 2]
        pltpu.make_async_copy(less, less, recv_b.at[2]).wait()

    spread_part(2)

    def exchange(t):
        way = (1 - 2 * lax.rem(t, 2)) * (1 - 2 * lax.rem(lax.div(t, subs), 2))
        return pltpu.make_async_remote_copy(
            src_ref=parts.at[t],
            dst_ref=got.at[t],
            send_sem=send_sem.at[t],
            recv_sem=recv_sem.at[t],
            device_id={"dir": lax.rem(row + way + 4, 4)},
            device_id_type=MESH,
        )

    wide = NB // HALF

    def pack(t, sums):
        for r in range(COEFFS // 8):
            for c in range(wide):
                parts[t, r * wide + c] = sums[r * 8 : r * 8 + 8, c * HALF : (c + 1) * HALF].astype(BF16)
        end = [sums[COEFFS - 1 : COEFFS, c * HALF : (c + 1) * HALF] for c in range(wide)]
        parts[t, COEFFS // 8 * wide] = jnp.concatenate(end * (8 // wide), axis=0).astype(BF16)

    def unpack(t):
        tiles = [got[t, i].astype(F32) for i in range(COEFFS // 8 * wide + 1)]
        rows = [jnp.concatenate(tiles[r * wide : (r + 1) * wide], axis=1) for r in range(COEFFS // 8)]
        end = jnp.concatenate([tiles[-1][c : c + 1] for c in range(wide)], axis=1)
        return jnp.concatenate(rows + [jnp.broadcast_to(end, (8, NB))], axis=0)

    def step(t, carry):
        base = lax.div(first_of(t), HALF)
        for n in range(NB // NI):
            cols = slice(n * NI, (n + 1) * NI)
            held, code = weight[t, :, cols], slot[t, :, cols]
            bounce = None
            for s in range(SLOTS):
                spread = jnp.where(code == jnp.int16(s), held, jnp.zeros_like(held))
                term = jnp.dot(matrix[s], spread, preferred_element_type=F32)
                bounce = term if bounce is None else bounce + term
            gain = SCALE * across(albedo_ref, base + n * (NI // HALF))
            total[:, cols] = direct[t, :, cols] + gain * bounce

        @pl.when(t < 2 * subs)
        def _():
            pack(t, total[:SEND])
            exchange(t).start()

        @pl.when(lax.div(t, subs) == 2)
        def _():
            exchange(t - 2 * subs).wait_recv()
            pack(t, total[:SEND] + unpack(t - 2 * subs))
            exchange(t).start()

        @pl.when(t >= 3 * subs)
        def _():
            own[t - 3 * subs] = total[:SEND]

        return carry

    lax.fori_loop(0, steps, step, 0)
    for i in range(subs):
        exchange(subs + i).wait_recv()
        exchange(2 * subs + i).wait_recv()
        mine = own[i] + unpack(subs + i) + unpack(2 * subs + i)
        begin = ((i % 2) * (subs // 2) + i // 2) * NB
        out_ref[:, begin : begin + NB] = mine[:COEFFS].astype(BF16)
    for t in range(3 * subs):
        exchange(t).wait_send()


def per_device(
    ray_code, occluder_list, list_count, normal_azimuth, normal_height, albedo, occluder_exit_radiance
):
    harmonics, axes = direction_tables()
    high = harmonics.astype(BF16)
    harmonics = np.concatenate([high, (harmonics - high.astype(np.float32)).astype(BF16)], axis=1)
    hbm = pl.BlockSpec(memory_space=pltpu.HBM)
    tiles = COEFFS // 8 * (NB // HALF) + 1
    steps = VERTS // NB
    sends = 3 * (OWN // NB)
    by_lane = (VERTS // HALF, HALF)
    dma = pltpu.SemaphoreType.DMA
    held = [
        pltpu.with_memory_space_constraint(a, pltpu.HBM)
        for a in (
            ray_code,
            list_count,
            occluder_exit_radiance.transpose(1, 0, 2),
            occluder_list.T,
            jnp.asarray(axes),
            normal_azimuth.reshape(by_lane),
            normal_height.reshape(by_lane),
            albedo.reshape(by_lane),
            jnp.asarray(harmonics),
        )
    ]
    return pl.pallas_call(
        transfer_kernel,
        out_shape=jax.ShapeDtypeStruct((COEFFS, OWN), BF16),
        in_specs=[hbm] * 9,
        out_specs=pl.BlockSpec(memory_space=pltpu.VMEM),
        scratch_shapes=[
            pltpu.SMEM((CLUSTERS,), jnp.int32),
            pltpu.VMEM((SLOTS, CLUSTERS), jnp.int32),
            pltpu.VMEM((DIRS, 8), F32),
            pltpu.VMEM(by_lane, F32),
            pltpu.VMEM(by_lane, F32),
            pltpu.VMEM(by_lane, F32),
            pltpu.VMEM((2 * ROWS, DIRS), BF16),
            pltpu.VMEM((steps, DIRS, NB), jnp.int32),
            pltpu.VMEM((steps, DIRS, NB), BF16),
            pltpu.VMEM((steps, DIRS, NB), jnp.int16),
            pltpu.VMEM((steps, ROWS, NB), F32),
            pltpu.VMEM((ROWS, NB), F32),
            pltpu.VMEM((OWN // NB, SEND, NB), F32),
            pltpu.VMEM((2,) + by_lane, F32),
            pltpu.VMEM((CLUSTERS * SLOTS, CLUSTERS * BLK), BF16),
            pltpu.VMEM((SLOTS * KG, SLOTS * KG), BF16),
            pltpu.VMEM((COEFFS, BLK, DIRS), BF16),
            pltpu.VMEM((CLUSTERS, PARTS, BLK, HALF), BF16),
            pltpu.VMEM((CLUSTERS, PARTS, SLOTS, HALF), BF16),
            pltpu.VMEM((2, KG, PARTS, SLOTS, HALF), BF16),
            pltpu.VMEM((SLOTS, ROWS, DIRS), BF16),
            pltpu.VMEM((sends, tiles, 8, HALF), BF16),
            pltpu.VMEM((sends, tiles, 8, HALF), BF16),
            dma((8,)),
            dma((steps,)),
        ]
        + [dma((PARTS,))] * 4
        + [dma((sends,)), dma((sends,))],
        compiler_params=pltpu.CompilerParams(
            collective_id=0, has_side_effects=True, vmem_limit_bytes=40 << 20
        ),
        name="transfer",
    )(*held)


def solution(mesh):
    return jax.shard_map(
        per_device,
        mesh=mesh,
        in_specs=(
            P("dir", "cluster"),
            P(),
            P(),
            P("cluster"),
            P("cluster"),
            P("cluster"),
            P("cluster", None, "dir"),
        ),
        out_specs=P(None, ("cluster", "dir")),
        check_vma=False,
    )
```

```python
import math

import jax
import jax.numpy as jnp
import numpy as np
from jax import lax
from jax.experimental import pallas as pl
from jax.experimental.pallas import tpu as pltpu
from jax.sharding import PartitionSpec as P

NDIR = 1024
SHORD = 9
COEFFS = 81
SLOTS = 16
CLUSTERS = 64
BLK = 8
DIRS = 256
HALF = 128
VERTS = 8192
OWN = 2048
KG = 32
PARTS = 3
ROWS = KG * PARTS
SEND = 88
FULL = COEFFS - KG * (PARTS - 1)
NB = 512
NI = 256
F32 = jnp.float32
BF16 = jnp.bfloat16
MESH = pl.DeviceIdType.MESH
SCALE = 4.0 * math.pi / NDIR
GOLDEN = math.pi * (3.0 - math.sqrt(5.0))


def direction_tables():
    p = np.arange(NDIR, dtype=np.float32)
    z = (np.float32(1.0) - (np.float32(2.0) * p + np.float32(1.0)) / np.float32(NDIR)).astype(np.float32)
    r = np.sqrt(np.maximum(np.float32(1.0) - z * z, np.float32(0.0)))
    t = (p * np.float32(GOLDEN)).astype(np.float64)
    x = (r * np.cos(t).astype(np.float32)).astype(np.float64)
    y = (r * np.sin(t).astype(np.float32)).astype(np.float64)
    z = z.astype(np.float64)
    c, s = [np.ones_like(x)], [np.zeros_like(x)]
    for _ in range(1, SHORD):
        c.append(c[-1] * x - s[-1] * y)
        s.append(c[-2] * y + s[-1] * x)
    rows = [None] * COEFFS
    for m in range(SHORD):
        q = [None] * SHORD
        q[m] = np.full_like(z, float(np.prod(np.arange(1, 2 * m, 2, dtype=np.float64))))
        if m + 1 < SHORD:
            q[m + 1] = z * (2 * m + 1) * q[m]
        for l in range(m + 2, SHORD):
            q[l] = ((2 * l - 1) * z * q[l - 1] - (l + m - 1) * q[l - 2]) / (l - m)
        for l in range(m, SHORD):
            n = math.sqrt((2 * l + 1) / (4.0 * math.pi) * math.factorial(l - m) / math.factorial(l + m))
            at = l * l + l
            if m == 0:
                rows[at] = n * q[l]
            else:
                rows[at + m] = math.sqrt(2.0) * n * q[l] * c[m]
                rows[at - m] = math.sqrt(2.0) * n * q[l] * s[m]
    table = np.zeros((4, ROWS, DIRS), np.float32)
    table[:, :COEFFS] = np.stack(rows).reshape(COEFFS, 4, DIRS).transpose(1, 0, 2)
    axes = np.zeros((4, DIRS, 8), np.float32)
    for i, a in enumerate((x, y, z)):
        axes[:, :, i] = a.reshape(4, DIRS)
    return table, axes


def place(x, z, core):
    return core, lax.rem((z * 4 + x) * 5, KG)


def transfer_kernel(
    code_ref, count_hbm, block_hbm, list_hbm, axes_hbm, azimuth_hbm, height_hbm, albedo_hbm, harm_hbm, out_ref,
    count_ref, list_ref, axes_ref, azimuth_ref, height_ref, albedo_ref, harm_ref, codes, weight, slot, direct, total, own, normal, chosen, turn, blocks, slices, picked, table, matrix, parts, got,
    load_sem, code_sem, send_a, recv_a, send_b, recv_b, send_sem, recv_sem,
):
    me = lax.axis_index("cluster")
    row = lax.axis_index("dir")
    my_x, my_z, my_core = lax.div(me, 16), lax.rem(lax.div(me, 2), 8), lax.rem(me, 2)
    my_half, my_group = place(my_x, my_z, my_core)
    steps = VERTS // NB
    subs = OWN // NB

    columns = [lax.rem(my_x + i, 4) for i in range(4)]
    cores = [my_core, 1 - my_core]

    def each_peer(act):
        def visit(j, carry):
            z = lax.rem(my_z + 4 + lax.div(j + 1, 2) * (1 - 2 * lax.rem(j, 2)), 8)
            for dx in (2, 1, 3, 0):
                for flip in (1, 0):
                    if dx or flip:
                        act((columns[dx], z, cores[flip]))
                    else:

                        @pl.when(j < 7)
                        def _():
                            act((columns[0], z, cores[0]))

            return carry

        lax.fori_loop(0, 8, visit, 0)

    def at(x, z, core):
        return {"cluster": x * 16 + z * 2 + core}

    def first_of(t):
        pair, half = lax.div(t, subs), lax.rem(t, 2)
        ahead = lax.rem(2 + pair, 4) + lax.div(pair, 2) * (1 - 2 * lax.rem(pair, 2))
        ahead = ahead + 2 * half * lax.rem(lax.div(pair + 1, 2), 2)
        inner = half * (subs // 2) + lax.rem(lax.div(t, 2), subs // 2)
        return pl.multiple_of(lax.rem(row + ahead, 4) * OWN + inner * NB, NB)

    def fetch(t):
        return pltpu.make_async_copy(code_ref.at[:, pl.ds(first_of(t), NB)], codes.at[t], code_sem.at[t])

    loads = [
        pltpu.make_async_copy(source, target, load_sem.at[i])
        for i, (source, target) in enumerate(
            (
                (block_hbm, blocks),
                (count_hbm, count_ref),
                (list_hbm, list_ref),
                (azimuth_hbm, azimuth_ref),
                (height_hbm, height_ref),
                (albedo_hbm, albedo_ref),
                (axes_hbm.at[row], axes_ref),
                (harm_hbm.at[row], harm_ref),
            )
        )
    ]
    barrier = pltpu.get_barrier_semaphore()

    def greet(peer):
        pl.semaphore_signal(barrier, inc=1, device_id=at(*peer), device_id_type=MESH)

    each_peer(greet)
    for i in (1, 3):
        pl.semaphore_signal(barrier, inc=1, device_id={"dir": lax.rem(row + i, 4)}, device_id_type=MESH)

    for load in loads:
        load.start()

    def start_fetch(t, carry):
        fetch(t).start()
        return carry

    lax.fori_loop(0, steps, start_fetch, 0)

    for load in loads:
        load.wait()
    my_lanes = pl.ds(pl.multiple_of(my_half * HALF, HALF), HALF)
    for unit in range(PARTS - 1):
        slices[me, unit] = blocks[unit * KG + my_group, :, my_lanes]

    @pl.when(my_group < FULL)
    def _():
        slices[me, PARTS - 1] = blocks[(PARTS - 1) * KG + my_group, :, my_lanes]

    lists = jnp.broadcast_to(list_ref[...].astype(F32).T[:, None, :], (CLUSTERS, SLOTS, SLOTS))
    here = lax.broadcasted_iota(jnp.int32, lists.shape, 1) == lax.broadcasted_iota(jnp.int32, lists.shape, 2)
    column = jnp.sum(jnp.where(here, lists, 0.0), axis=2, keepdims=True).reshape(CLUSTERS * SLOTS, 1)
    each = lax.broadcasted_iota(jnp.int32, (CLUSTERS * SLOTS, CLUSTERS * BLK), 1).astype(F32)
    chosen[...] = jnp.where(column == each, 1.0, 0.0).astype(BF16)
    to = lax.broadcasted_iota(jnp.int32, (SLOTS * KG, SLOTS * KG), 0)
    fro = lax.broadcasted_iota(jnp.int32, (SLOTS * KG, SLOTS * KG), 1)
    turn[...] = jnp.where((to % KG) * SLOTS + to // KG == fro, 1.0, 0.0).astype(BF16)
    table[:, FULL:, PARTS - 1] = jnp.zeros((2, KG - FULL, SLOTS, HALF), BF16)
    height = height_ref[...]
    planar = jnp.sqrt(jnp.maximum(1.0 - height * height, 0.0))
    normal[0] = planar * jnp.cos(azimuth_ref[...])
    normal[1] = planar * jnp.sin(azimuth_ref[...])
    pl.semaphore_wait(barrier, CLUSTERS + 1)

    def first(peer, unit):
        half, group = place(*peer)
        return pltpu.make_async_remote_copy(
            src_ref=blocks.at[unit * KG + group, :, pl.ds(pl.multiple_of(half * HALF, HALF), HALF)],
            dst_ref=slices.at[me, unit],
            send_sem=send_a.at[unit],
            recv_sem=recv_a.at[unit],
            device_id=at(*peer),
            device_id_type=MESH,
        )

    def start_first(peer):
        first(peer, 0).start()

    def start_first_rest(peer):
        first(peer, 1).start()

        @pl.when(place(*peer)[1] < FULL)
        def _():
            first(peer, 2).start()

    each_peer(start_first)
    each_peer(start_first_rest)

    count = count_ref[me]
    x, y, z = (axes_ref[:, i : i + 1] for i in range(3))

    def across(ref, at):
        return jnp.concatenate([ref[pl.ds(at + i, 1), :] for i in range(NI // HALF)], axis=1)

    def prepare(t, carry):
        fetch(t).wait()
        base = lax.div(first_of(t), HALF)
        for n in range(NB // NI):
            cols = slice(n * NI, (n + 1) * NI)
            at = base + n * (NI // HALF)
            code = codes[t, :, cols]
            facing = jnp.maximum(
                x * across(normal.at[0], at) + y * across(normal.at[1], at) + z * across(height_ref, at), 0.0
            )
            hit = code < count
            weight[t, :, cols] = facing.astype(BF16)
            slot[t, :, cols] = jnp.where(hit, code, SLOTS).astype(jnp.int16)
            lit = jnp.where(hit, 0.0, facing)
            high = lit.astype(BF16)
            low = (lit - high.astype(F32)).astype(BF16)
            both = jnp.dot(harm_ref[...], high, preferred_element_type=F32)
            rest = jnp.dot(harm_ref[:ROWS], low, preferred_element_type=F32)
            direct[t, :, cols] = SCALE * (both[:ROWS] + both[ROWS:] + rest)
        return carry

    def choose(unit):
        others = slices.at[pl.ds(0, CLUSTERS - 1), unit]
        pltpu.make_async_copy(others, others, recv_a.at[unit]).wait()
        held = slices[:, unit].reshape(CLUSTERS * BLK, HALF)
        rows = jnp.dot(chosen[...], held, preferred_element_type=F32).astype(BF16)
        picked[:, unit] = rows.reshape(CLUSTERS, SLOTS, HALF)

    def second(unit):
        def start(peer):
            pltpu.make_async_remote_copy(
                src_ref=picked.at[at(*peer)["cluster"], unit],
                dst_ref=table.at[my_half, my_group, unit],
                send_sem=send_b.at[unit],
                recv_sem=recv_b.at[unit],
                device_id=at(*peer),
                device_id_type=MESH,
            ).start()

        each_peer(start)

    lax.fori_loop(0, 4, prepare, 0)
    choose(0)
    second(0)
    lax.fori_loop(4, 8, prepare, 0)
    choose(1)
    second(1)

    @pl.when(my_group < FULL)
    def _():
        choose(2)
        second(2)
        table[my_half, my_group, 2] = picked[me, 2]

    for unit in range(PARTS - 1):
        table[my_half, my_group, unit] = picked[me, unit]

    lax.fori_loop(8, steps, prepare, 0)

    def spread_part(i):
        both = jnp.concatenate([table[h, :, i].reshape(KG * SLOTS, HALF) for h in range(2)], axis=1)
        turned = jnp.dot(turn[...], both, preferred_element_type=F32).astype(BF16)
        matrix[:, i * KG : (i + 1) * KG, :] = turned.reshape(SLOTS, KG, DIRS)

    for unit in range(PARTS - 1):
        sent = picked.at[pl.ds(0, CLUSTERS - 1), unit]
        pltpu.make_async_copy(sent, sent, recv_b.at[unit]).wait()
        spread_part(unit)

    @pl.when(my_group < FULL)
    def _():
        less = picked.at[pl.ds(0, 2 * FULL - 1), 2]
        pltpu.make_async_copy(less, less, recv_b.at[2]).wait()

    @pl.when(my_group >= FULL)
    def _():
        less = picked.at[pl.ds(0, 2 * FULL), 2]
        pltpu.make_async_copy(less, less, recv_b.at[2]).wait()

    spread_part(2)

    def exchange(t):
        way = (1 - 2 * lax.rem(t, 2)) * (1 - 2 * lax.rem(lax.div(t, subs), 2))
        return pltpu.make_async_remote_copy(
            src_ref=parts.at[t],
            dst_ref=got.at[t],
            send_sem=send_sem.at[t],
            recv_sem=recv_sem.at[t],
            device_id={"dir": lax.rem(row + way + 4, 4)},
            device_id_type=MESH,
        )

    wide = NB // HALF

    def pack(t, sums):
        for r in range(COEFFS // 8):
            for c in range(wide):
                parts[t, r * wide + c] = sums[r * 8 : r * 8 + 8, c * HALF : (c + 1) * HALF].astype(BF16)
        end = [sums[COEFFS - 1 : COEFFS, c * HALF : (c + 1) * HALF] for c in range(wide)]
        parts[t, COEFFS // 8 * wide] = jnp.concatenate(end * (8 // wide), axis=0).astype(BF16)

    def unpack(t):
        tiles = [got[t, i].astype(F32) for i in range(COEFFS // 8 * wide + 1)]
        rows = [jnp.concatenate(tiles[r * wide : (r + 1) * wide], axis=1) for r in range(COEFFS // 8)]
        end = jnp.concatenate([tiles[-1][c : c + 1] for c in range(wide)], axis=1)
        return jnp.concatenate(rows + [jnp.broadcast_to(end, (8, NB))], axis=0)

    def step(t, carry):
        base = lax.div(first_of(t), HALF)
        for n in range(NB // NI):
            cols = slice(n * NI, (n + 1) * NI)
            held, code = weight[t, :, cols], slot[t, :, cols]
            bounce = None
            for s in range(SLOTS):
                spread = jnp.where(code == jnp.int16(s), held, jnp.zeros_like(held))
                term = jnp.dot(matrix[s], spread, preferred_element_type=F32)
                bounce = term if bounce is None else bounce + term
            gain = SCALE * across(albedo_ref, base + n * (NI // HALF))
            total[:, cols] = direct[t, :, cols] + gain * bounce

        @pl.when(t < 2 * subs)
        def _():
            pack(t, total[:SEND])
            exchange(t).start()

        @pl.when(lax.div(t, subs) == 2)
        def _():
            exchange(t - 2 * subs).wait_recv()
            pack(t, total[:SEND] + unpack(t - 2 * subs))
            exchange(t).start()

        @pl.when(t >= 3 * subs)
        def _():
            own[t - 3 * subs] = total[:SEND]

        return carry

    lax.fori_loop(0, steps, step, 0)
    for i in range(subs):
        exchange(subs + i).wait_recv()
        exchange(2 * subs + i).wait_recv()
        mine = own[i] + unpack(subs + i) + unpack(2 * subs + i)
        begin = ((i % 2) * (subs // 2) + i // 2) * NB
        out_ref[:, begin : begin + NB] = mine[:COEFFS].astype(BF16)
    for t in range(3 * subs):
        exchange(t).wait_send()
    for unit in range(PARTS - 1):
        others = slices.at[pl.ds(0, CLUSTERS - 1), unit]
        sent = picked.at[pl.ds(0, CLUSTERS - 1), unit]
        pltpu.make_async_copy(others, others, send_a.at[unit]).wait()
        pltpu.make_async_copy(sent, sent, send_b.at[unit]).wait()

    @pl.when(my_group < FULL)
    def _():
        fewer = slices.at[pl.ds(0, 2 * FULL - 1), 2]
        pltpu.make_async_copy(fewer, fewer, send_a.at[2]).wait()
        tail = picked.at[pl.ds(0, CLUSTERS - 1), 2]
        pltpu.make_async_copy(tail, tail, send_b.at[2]).wait()

    @pl.when(my_group >= FULL)
    def _():
        fewer = slices.at[pl.ds(0, 2 * FULL), 2]
        pltpu.make_async_copy(fewer, fewer, send_a.at[2]).wait()


def per_device(
    ray_code, occluder_list, list_count, normal_azimuth, normal_height, albedo, occluder_exit_radiance
):
    harmonics, axes = direction_tables()
    high = harmonics.astype(BF16)
    harmonics = np.concatenate([high, (harmonics - high.astype(np.float32)).astype(BF16)], axis=1)
    hbm = pl.BlockSpec(memory_space=pltpu.HBM)
    tiles = COEFFS // 8 * (NB // HALF) + 1
    steps = VERTS // NB
    sends = 3 * (OWN // NB)
    by_lane = (VERTS // HALF, HALF)
    dma = pltpu.SemaphoreType.DMA
    held = [
        pltpu.with_memory_space_constraint(a, pltpu.HBM)
        for a in (
            ray_code,
            list_count,
            occluder_exit_radiance.transpose(1, 0, 2),
            occluder_list.T,
            jnp.asarray(axes),
            normal_azimuth.reshape(by_lane),
            normal_height.reshape(by_lane),
            albedo.reshape(by_lane),
            jnp.asarray(harmonics),
        )
    ]
    return pl.pallas_call(
        transfer_kernel,
        out_shape=jax.ShapeDtypeStruct((COEFFS, OWN), BF16),
        in_specs=[hbm] * 9,
        out_specs=pl.BlockSpec(memory_space=pltpu.VMEM),
        scratch_shapes=[
            pltpu.SMEM((CLUSTERS,), jnp.int32),
            pltpu.VMEM((SLOTS, CLUSTERS), jnp.int32),
            pltpu.VMEM((DIRS, 8), F32),
            pltpu.VMEM(by_lane, F32),
            pltpu.VMEM(by_lane, F32),
            pltpu.VMEM(by_lane, F32),
            pltpu.VMEM((2 * ROWS, DIRS), BF16),
            pltpu.VMEM((steps, DIRS, NB), jnp.int32),
            pltpu.VMEM((steps, DIRS, NB), BF16),
            pltpu.VMEM((steps, DIRS, NB), jnp.int16),
            pltpu.VMEM((steps, ROWS, NB), F32),
            pltpu.VMEM((ROWS, NB), F32),
            pltpu.VMEM((OWN // NB, SEND, NB), F32),
            pltpu.VMEM((2,) + by_lane, F32),
            pltpu.VMEM((CLUSTERS * SLOTS, CLUSTERS * BLK), BF16),
            pltpu.VMEM((SLOTS * KG, SLOTS * KG), BF16),
            pltpu.VMEM((COEFFS, BLK, DIRS), BF16),
            pltpu.VMEM((CLUSTERS, PARTS, BLK, HALF), BF16),
            pltpu.VMEM((CLUSTERS, PARTS, SLOTS, HALF), BF16),
            pltpu.VMEM((2, KG, PARTS, SLOTS, HALF), BF16),
            pltpu.VMEM((SLOTS, ROWS, DIRS), BF16),
            pltpu.VMEM((sends, tiles, 8, HALF), BF16),
            pltpu.VMEM((sends, tiles, 8, HALF), BF16),
            dma((8,)),
            dma((steps,)),
        ]
        + [dma((PARTS,))] * 4
        + [dma((sends,)), dma((sends,))],
        compiler_params=pltpu.CompilerParams(
            collective_id=0, has_side_effects=True, vmem_limit_bytes=40 << 20
        ),
        name="transfer",
    )(*held)


def solution(mesh):
    return jax.shard_map(
        per_device,
        mesh=mesh,
        in_specs=(
            P("dir", "cluster"),
            P(),
            P(),
            P("cluster"),
            P("cluster"),
            P("cluster"),
            P("cluster", None, "dir"),
        ),
        out_specs=P(None, ("cluster", "dir")),
        check_vma=False,
    )
```
